256 devices in a mesh: gy: 64 (over z, y_lo, x), gx: 4 (over y_hi, core).
Axes of the slice: x: 4, y: 4 (y_hi: 2, y_lo: 2; y = y_hi * 2 + y_lo), z: 8, core: 2. Of those that a mesh axis runs over, the one named last changes fastest.
Arguments:
- fields: float32 [8, 64, 2048, 128], P(None, 'gx', 'gy'), may hold values from -6 to 6
- shifts: int32 [64], P('gx'), may hold values from 0 to 2047
- fraction: float32 [64], P('gx'), may hold values from 0.4 to 0.6
Outputs:
- remapped: float32 [8, 64, 2048, 128], P(None, 'gx', 'gy')
- stress: float32 [2, 128], replicated
The draws below stay inside these ranges and needn't reach their ends.
All inputs are finite; a program needn't handle non-finite values.
Results may differ from the reference program's by a relative error of at most 0.0003.
Values sent between devices are 32-bit elements; how exact they have to be, the bound alone decides.
No kernel may reach another device: no remote copies, remote signals or barrier semaphores. Data moves between devices by JAX's collectives and lax.ppermute only.
A program may use at most 64 MiB of HBM per device.

```python
import math
import jax
import jax.numpy as jnp
from jax import lax

FIELDS = 8
CZ = 128
NX = 64
NY = 2048


def draw_fields(key, part):
    key_rough = jax.random.fold_in(key, 11)
    key_level = jax.random.fold_in(key, 12)
    rough_part = jnp.clip(jax.random.normal(key_rough, (FIELDS, NX, NY, CZ), jnp.float32), -5.0, 5.0)
    amplitude = jax.random.uniform(key_level, (2, NX, 1, CZ), jnp.float32, 0.3, 0.6)
    parity = 1.0 - 2.0 * (jnp.arange(NY) % 2).astype(jnp.float32)
    alternating = amplitude * parity[None, None, :, None]
    component = jnp.arange(FIELDS)
    first_pair = ((component == 1) | (component == 2)).astype(jnp.float32)
    second_pair = ((component == 5) | (component == 6)).astype(jnp.float32)
    pattern = first_pair[:, None, None, None] * alternating[0][None] + second_pair[:, None, None, None] * alternating[1][None]
    return rough_part + pattern


def place_ends(array, key, smallest, high):
    longest = array.shape.index(max(array.shape))
    spots = []
    for shift in (0, 1):
        where = [jax.random.randint(jax.random.fold_in(key, axis), (), 0, length) for axis, length in enumerate(array.shape)]
        where[longest] = (where[longest] + shift) % array.shape[longest]
        spots.append(tuple(where))
    return array.at[spots[0]].set(smallest).at[spots[1]].set(high)


def steps_of(key, dims, shards, least, high):
    gain, own = 1.0, jax.random.fold_in(key, 6)
    for axis_at, blocks in shards:
        steps = jnp.exp(jax.random.uniform(jax.random.fold_in(own, axis_at), (blocks,), jnp.float32, least / len(shards), high / len(shards)))
        gain = gain * jnp.repeat(steps, dims[axis_at] // blocks).reshape([-1 if axis == axis_at else 1 for axis in range(len(dims))])
    return gain


def setup_inputs(seed: int = 0) -> dict:
    key_of = jax.random.split(jax.random.key(seed), 4)
    return {
        "fields": draw_fields(jax.random.fold_in(key_of[3], 71), 0),
        "shifts": place_ends(jax.random.randint(key_of[1], (NX,), 0, NY), jax.random.fold_in(key_of[1], 1), 0, NY - 1).astype(jnp.int32),
        "fraction": jnp.clip(0.4 + 0.20000002 * jax.random.uniform(key_of[2], (NX,), jnp.float32) ** steps_of(key_of[2], (NX,), ((0, 4),), -0.2, 0.2), 0.4, 0.6),
    }


def remap_cells(extended, fraction, length, stride):

    def cells(first, number):
        return extended[..., first * stride:(first + number) * stride]
    interface = (7.0 * (cells(1, length + 2) + cells(2, length + 2)) - (cells(0, length + 2) + cells(3, length + 2))) / 12.0
    left_edge = interface[..., :(length + 1) * stride]
    right_edge = interface[..., stride:]
    centre = cells(2, length + 1)
    slope = right_edge - left_edge
    curve = 6.0 * centre - 3.0 * (left_edge + right_edge)
    outflow = fraction * (right_edge - 0.5 * fraction * (slope - (1.0 - 2.0 * fraction / 3.0) * curve))
    return cells(3, length) - outflow[..., stride:] + outflow[..., :length * stride]

def reference(fields, shifts, fraction):

    def one_column(items):
        column, shift, share = items
        start = jnp.mod(-3 - shift, NY).astype(jnp.int32)
        doubled = jnp.concatenate([column, column, column[:, :4, :]], axis=1)
        extended = lax.dynamic_slice_in_dim(doubled, start, NY + 5, 1)
        flat = extended.reshape(FIELDS, (NY + 5) * CZ)
        return remap_cells(flat, share, NY, CZ).reshape(FIELDS, NY, CZ)
    moved = lax.map(one_column, (jnp.moveaxis(fields, 1, 0), shifts, fraction))
    remapped = jnp.moveaxis(moved, 0, 1)
    reynolds = lax.optimization_barrier(jnp.sum(remapped[1] * remapped[2], axis=(0, 1)))
    maxwell = -lax.optimization_barrier(jnp.sum(remapped[5] * remapped[6], axis=(0, 1)))
    stress = jnp.stack([reynolds, maxwell]) / math.sqrt(NX * NY)
    return (remapped, stress)
```

```python
from functools import partial
import math

import jax
import jax.numpy as jnp
from jax import lax
from jax.experimental import pallas as pl
from jax.experimental.pallas import tpu as pltpu
from jax.sharding import Mesh
from jax.sharding import PartitionSpec as P

GY = ("gy_0", "gy_1", "gy_2")
GX = ("gx_0", "gx_1")
PAD = 48
SCOPE = 16 << 20


def taps(c):
    h = 0.5 * c
    m = 1.0 - (2.0 / 3.0) * c
    right = c * (1.0 - h - 3.0 * h * m)
    left = c * (h - 3.0 * h * m)
    here = 6.0 * c * h * m
    a, b = 1.0 / 12.0, 7.0 / 12.0
    both = right - left
    return (
        -a * left,
        b * left - a * both,
        here + a * right + b * both + b * left,
        (1.0 - here) - b * right + b * both - a * left,
        -b * right - a * both,
        a * right,
    )


def field_of(team, member):
    return jnp.where(team < 2, 4 * team + 1 + member, 4 * (team - 2) + 3 * member)


def copy_block(source, target):
    target[...] = source[...].reshape(target.shape)


def pack(fields):
    _, columns, slab, vertical = fields.shape
    return pl.pallas_call(
        copy_block,
        grid=(4, 2),
        in_specs=[pl.BlockSpec((1, columns, slab, vertical), lambda t, m: (field_of(t, m), 0, 0, 0))],
        out_specs=pl.BlockSpec((1, columns, 1, slab, vertical), lambda t, m: (t, 0, m, 0, 0)),
        out_shape=jax.ShapeDtypeStruct((4, columns, 2, slab, vertical), fields.dtype),
        compiler_params=pltpu.CompilerParams(vmem_limit_bytes=SCOPE),
        name="pack",
    )(fields)


def unpack(packed):
    _, columns, _, slab, vertical = packed.shape
    return pl.pallas_call(
        copy_block,
        grid=(4, 2),
        in_specs=[pl.BlockSpec((1, columns, 1, slab, vertical), lambda t, m: (t, 0, m, 0, 0))],
        out_specs=pl.BlockSpec((1, columns, slab, vertical), lambda t, m: (field_of(t, m), 0, 0, 0)),
        out_shape=jax.ShapeDtypeStruct((8, columns, slab, vertical), packed.dtype),
        compiler_params=pltpu.CompilerParams(vmem_limit_bytes=SCOPE),
        name="unpack",
    )(packed)


def remap_kernel(place_ref, shifts_ref, fraction_ref, held_ref, moved_ref, sums_ref, column_ref):
    slabs, members, slab, vertical = held_ref.shape
    azimuth = slabs * slab
    place = place_ref[0]
    column = lax.rem(place, shifts_ref.shape[0])
    team = lax.div(place, shifts_ref.shape[0])
    shift = shifts_ref[column]
    weights = taps(fraction_ref[column])

    def fill(g, carry):
        for m in range(members):
            column_ref[m, pl.ds(pl.multiple_of(g * slab, slab), slab), :] = held_ref[g, m]
        return carry

    lax.fori_loop(0, slabs, fill, 0, unroll=4)
    for m in range(members):
        column_ref[m, azimuth : azimuth + slab, :] = held_ref[0, m]
        column_ref[m, azimuth + slab : azimuth + PAD, :] = held_ref[1, m, : PAD - slab]

    def remap(g, total):
        start = lax.rem(g * slab - shift - 3 + 2 * azimuth, azimuth)
        for r in range(0, slab, 8):
            both = []
            for m in range(members):
                value = weights[0] * column_ref[m, pl.ds(start + r, 8), :]
                for k in range(1, 6):
                    value += weights[k] * column_ref[m, pl.ds(start + r + k, 8), :]
                moved_ref[g, m, r : r + 8, :] = value
                both.append(value)
            total += both[0] * both[1]
        return total

    total = lax.fori_loop(0, slabs, remap, jnp.zeros((8, vertical), jnp.float32), unroll=2)
    product = jnp.sum(total, axis=0, keepdims=True)
    sums_ref[0:1, :] = jnp.where(team == 0, product, 0.0)
    sums_ref[1:2, :] = jnp.where(team == 1, -product, 0.0)


def remap(place, shifts, fraction, held):
    slabs, members, slab, vertical = held.shape
    smem = pl.BlockSpec(memory_space=pltpu.SMEM)
    vmem = pl.BlockSpec(memory_space=pltpu.VMEM)
    return pl.pallas_call(
        remap_kernel,
        in_specs=[smem, smem, smem, vmem],
        out_specs=[vmem, vmem],
        out_shape=[
            jax.ShapeDtypeStruct(held.shape, held.dtype),
            jax.ShapeDtypeStruct((2, vertical), jnp.float32),
        ],
        scratch_shapes=[pltpu.VMEM((members, slabs * slab + PAD, vertical), jnp.float32)],
        compiler_params=pltpu.CompilerParams(vmem_limit_bytes=SCOPE),
        name="remap",
    )(place, shifts, fraction, held)


def on_device(fields, shifts, fraction):
    components, columns, slab, vertical = fields.shape
    slabs = lax.axis_size(GY)
    place = lax.axis_index(GY).astype(jnp.int32).reshape(1)
    packed = pack(fields).reshape(components * columns, slab, vertical)
    held = lax.all_to_all(packed, GY, split_axis=0, concat_axis=0, tiled=True)
    moved, sums = remap(place, shifts, fraction, held.reshape(slabs, 2, slab, vertical))
    returned = lax.all_to_all(
        moved.reshape(components * columns, slab, vertical), GY, split_axis=0, concat_axis=0, tiled=True
    )
    remapped = unpack(returned.reshape(4, columns, 2, slab, vertical))
    for axis in GY + GX:
        sums = lax.psum(sums, axis)
    cells = columns * lax.axis_size(GX) * slab * slabs
    return remapped, sums / math.sqrt(cells)


def solution(mesh):
    split = Mesh(mesh.devices.reshape(8, 2, 4, 2, 2), GY + GX)
    placed = (P(None, GX, GY, None), P(GX), P(GX))
    return jax.shard_map(
        on_device,
        mesh=split,
        in_specs=placed,
        out_specs=(P(None, GX, GY, None), P()),
        check_vma=False,
    )
```
